512 devices in a mesh: grp: 8 (over x, core), pq: 64 (over y, z).
Axes of the slice: x: 4, y: 8, z: 8, core: 2. Of those that a mesh axis runs over, the one named last changes fastest.
Arguments:
- pair_blocks: bfloat16 [16, 1152, 128, 128], P('grp', 'pq'), may hold values from -6 to 6
- block_list: int32 [16, 1152], P('grp', 'pq'), may hold values from 0 to 2047, as said below
- block_count: int32 [16, 64], P('grp', 'pq'), may hold values from 1 to 18, as said below
- coef: bfloat16 [4096, 512], P('pq', 'grp'), may hold values from -0.09375 to 0.09375
Outputs:
- transformed: float32 [32, 512, 512], P('grp', 'pq')
The draws below stay inside these ranges and needn't reach their ends.
Inputs may be any that keep to these rules, and one draw needn't show every extreme that they name: `block_list`: within one row the ids are distinct, each in 0 to 2 * 32^2 - 1. `block_count`: in every row some device has exactly 18 live slots.
All inputs are finite; a program needn't handle non-finite values.
Results may differ from the reference program's by a relative error of at most 0.0042.
Values may be sent and summed in bfloat16 or wider, within the bound.
A program may use at most 64 MiB of HBM per device.

```python
import jax
import jax.numpy as jnp
from jax import lax

NAO = 4096
NMO = 512
TILE = 128
KL_PANEL = 2
PANELS = 2
SLOTS = 18
NKL = 32
N_GRP = 8
N_PQ = 64


def draw_block_list(key, part):
    total_rows = PANELS * N_GRP
    keys = jax.random.split(jax.random.fold_in(key, 11), total_rows)
    idents = KL_PANEL * (NAO // TILE) * (NAO // TILE)

    def one_row(row_key):
        return jax.random.permutation(row_key, idents)[:N_PQ * SLOTS]
    return jax.vmap(one_row)(keys).astype(jnp.int32)


def draw_block_count(key, part):
    total_rows = PANELS * N_GRP
    first_key, second_key, third_key = jax.random.split(jax.random.fold_in(key, 23), 3)
    low = max(SLOTS // 2, 1)
    high = max(SLOTS, low + 1)
    first = jax.random.randint(first_key, (total_rows, N_PQ), low, high)
    second = jax.random.randint(second_key, (total_rows, N_PQ), low, high)
    counts = 1 + first * second // SLOTS
    counts = jnp.minimum(counts, SLOTS)
    busiest = jax.random.randint(third_key, (total_rows, 1), 0, N_PQ)
    places = jnp.arange(N_PQ, dtype=jnp.int32)[None, :]
    counts = jnp.where(places == busiest, SLOTS, counts)
    return counts.astype(jnp.int32)


def shard_levels(stream_key, shape, cuts, smallest, high):
    loudness, own = 1.0, jax.random.fold_in(stream_key, 6)
    for position, shards_of in cuts:
        steps = jnp.exp(jax.random.uniform(jax.random.fold_in(own, position), (shards_of,), jnp.float32, smallest / len(cuts), high / len(cuts)))
        loudness = loudness * jnp.repeat(steps, shape[position] // shards_of).reshape([-1 if axis == position else 1 for axis in range(len(shape))])
    return loudness


def scatter_about(stream_key, shape, width, most, cuts=(), kind=jnp.bfloat16):
    factor_of = shard_levels(stream_key, shape, cuts, -0.22, 0.18) if cuts else 1.0
    entries = jax.random.normal(stream_key, shape, jnp.float32) * width * factor_of
    return jnp.minimum(jnp.maximum(entries, -most), most).astype(kind)


def setup_inputs(seed: int = 0) -> dict:
    key_list = jax.random.split(jax.random.key(seed), 5)
    return {
        "pair_blocks": scatter_about(key_list[0], (PANELS * N_GRP, N_PQ * SLOTS, TILE, TILE), 1.0, 6.0, ((0, 8), (1, 64))),
        "block_list": draw_block_list(jax.random.fold_in(key_list[4], 71), 0),
        "block_count": draw_block_count(jax.random.fold_in(key_list[4], 71), 0),
        "coef": scatter_about(key_list[3], (NAO, NMO), NAO ** -0.5, 0.09375, ((0, 64), (1, 8))),
    }


def reference(pair_blocks, block_list, block_count, coef):
    nblk = NAO // TILE
    per_kl = nblk * nblk

    def one_row(inputs):
        blocks, idents, counts = inputs

        def step(acc, slot):
            live = (slot % SLOTS) < counts[slot // SLOTS]

            def add(total):
                ident = idents[slot]
                which = (ident // per_kl).astype(jnp.int32)
                row_blk = ((ident // nblk) % nblk).astype(jnp.int32)
                col_blk = (ident % nblk).astype(jnp.int32)
                col_coef = lax.dynamic_slice_in_dim(coef, col_blk * TILE, TILE, 0)
                row_coef = lax.dynamic_slice_in_dim(coef, row_blk * TILE, TILE, 0)
                block = lax.dynamic_index_in_dim(blocks, slot, 0, keepdims=False)
                half = jnp.dot(block, col_coef, preferred_element_type=jnp.float32).astype(jnp.bfloat16)
                term = jnp.dot(row_coef.T, half, preferred_element_type=jnp.float32)
                current = lax.dynamic_index_in_dim(total, which, 0, keepdims=False)
                return lax.dynamic_update_index_in_dim(total, current + term, which, 0)

            return lax.cond(live, add, lambda total: total, acc), None

        start = jnp.zeros((KL_PANEL, NMO, NMO), jnp.float32)
        result, _ = lax.scan(step, start, jnp.arange(N_PQ * SLOTS, dtype=jnp.int32))
        return result

    rows = lax.map(one_row, (pair_blocks, block_list, block_count))
    return rows.reshape(NKL, NMO, NMO)
```

```python
import jax
import jax.numpy as jnp
from jax import lax
from jax.experimental import pallas as pl
from jax.experimental.pallas import tpu as pltpu
from jax.sharding import PartitionSpec as P

MESH = pl.DeviceIdType.MESH
SIDE = 8
HALF = SIDE // 2
TILE = 128
KL = 2
PLACE = (0, 1, 3, 5, 7, 6, 4, 2)


def remote(src, dst, send, recv, device):
    return pltpu.make_async_remote_copy(
        src_ref=src, dst_ref=dst, send_sem=send, recv_sem=recv, device_id=device, device_id_type=MESH
    )


def gather_kernel(coef_ref, out_ref, mine, raw, g_send, g_recv, a_send, a_recv, b_send, b_recv, d_send, d_recv):
    g, p = lax.axis_index("grp"), lax.axis_index("pq")
    core = g % 2
    y, z = p // SIDE, p % SIDE
    a = y * (1 - core) + z * core
    b = z * (1 - core) + y * core
    step_a = SIDE * (1 - core) + core
    step_b = (1 - core) + SIDE * core

    def at(a_to, b_to):
        return (g, a_to * step_a + b_to * step_b)

    grp_peers = [((g + j) % 8, p) for j in range(1, 8)]
    a_peers = [at((a + d) % SIDE, b) for d in (1, 7, 2, 6, 3, 5, 4)]
    right, left = at(a, (b + 1) % SIDE), at(a, (b + 7) % SIDE)
    partner = (g + 1 - 2 * core, p)

    barrier = pltpu.get_barrier_semaphore()
    peers = grp_peers + a_peers + [right, left]
    for device in peers:
        pl.semaphore_signal(barrier, inc=1, device_id=device, device_id_type=MESH)
    mine[...] = jnp.concatenate([coef_ref[...], coef_ref[...]], axis=1)
    raw[g] = mine[pl.ds(pl.multiple_of(core * 32, 32), 32), :]
    pl.semaphore_wait(barrier, len(peers))

    sent = []
    for j in range(1, 8):
        g_to = (g + j) % 8
        rows = pl.ds(pl.multiple_of((g_to % 2) * 32, 32), 32)
        copy = remote(mine.at[rows, :], raw.at[g], g_send.at[j], g_recv.at[j], (g_to, p))
        copy.start()
        sent.append(copy)
    for copy in sent:
        copy.wait_recv()
    low = lax.broadcasted_iota(jnp.int32, (32, TILE), 1) < TILE // 2
    for x in range(4):
        out_ref[core, b, 0, x] = jnp.where(low, raw[2 * x], raw[2 * x + 1])

    arrivals = {}
    for n, d in enumerate((1, 7, 2, 6, 3, 5, 4)):
        place = PLACE[(8 - d) % 8]
        copy = remote(out_ref.at[core, b, 0], out_ref.at[core, b, place], a_send.at[place], a_recv.at[place], a_peers[n])
        copy.start()
        sent.append(copy)
        arrivals[place] = copy

    def line(b_from, part):
        return out_ref.at[core, b_from, pl.ds(HALF * part, HALF)]

    def pass_on(way, part, step, b_from):
        block = line(b_from, part)
        hops = HALF if way == part else HALF - 1
        if step < hops:
            copy = remote(block, block, b_send.at[way, part, step], b_recv.at[way, part, step], (right, left)[way])
            copy.start()
            sent.append(copy)
            flights[way, part, step + 1] = copy
        if step > 0 or way == 0:
            n = (way * 2 + part) * (HALF + 1) + step
            copy = remote(block, block, d_send.at[n], d_recv.at[n], partner)
            copy.start()
            sent.append(copy)
            across.append(copy)

    flights, across = {}, []
    for part in range(2):
        for place in range(HALF * part, HALF * part + HALF):
            if place > 0:
                arrivals[place].wait_recv()
        for way in range(2):
            pass_on(way, part, 0, b)
    for step in range(1, HALF + 1):
        for part in range(2):
            for way in range(2):
                if (way, part, step) in flights:
                    flights[way, part, step].wait_recv()
                    away = step if way == 0 else 8 - step
                    pass_on(way, part, step, (b + 8 - away) % SIDE)
    for copy in across:
        copy.wait_recv()
    for copy in sent:
        copy.wait_send()


def gather(coef):
    return pl.pallas_call(
        gather_kernel,
        name="gather_coef",
        out_shape=jax.ShapeDtypeStruct((2, SIDE, SIDE, 4, 32, TILE), jnp.bfloat16),
        in_specs=[pl.BlockSpec(memory_space=pltpu.VMEM)],
        out_specs=pl.BlockSpec(memory_space=pltpu.VMEM),
        scratch_shapes=[
            pltpu.VMEM((64, TILE), jnp.bfloat16),
            pltpu.VMEM((8, 32, TILE), jnp.bfloat16),
            pltpu.SemaphoreType.DMA((8,)),
            pltpu.SemaphoreType.DMA((8,)),
            pltpu.SemaphoreType.DMA((8,)),
            pltpu.SemaphoreType.DMA((8,)),
            pltpu.SemaphoreType.DMA((2, 2, 4)),
            pltpu.SemaphoreType.DMA((2, 2, 4)),
            pltpu.SemaphoreType.DMA((20,)),
            pltpu.SemaphoreType.DMA((20,)),
        ],
        compiler_params=pltpu.CompilerParams(collective_id=0, has_side_effects=True),
    )(coef)


def transform_kernel(list_ref, count_ref, blocks_ref, coef_ref, out_ref, half_ref, left_ref):
    p = lax.axis_index("pq")
    y_me, z_me = p // SIDE, p % SIDE
    slots = blocks_ref.shape[1]
    nblk = SIDE * SIDE // 2

    def place(k):
        k = (k + SIDE) % SIDE
        return jnp.where(k == 0, 0, jnp.where(k <= HALF, 2 * k - 1, 16 - 2 * k))

    def rows_of(tile):
        parts = []
        for e in range(2):
            y, z = tile // 4, 2 * (tile % 4) + e
            parts.append(coef_ref[0, z, place(y - y_me)])
            parts.append(coef_ref[1, y, place(z - z_me)])
        return [jnp.concatenate([part[x] for part in parts], axis=0) for x in range(4)]

    for panel in range(2):

        def one_slot(slot, carry):
            ident = list_ref[panel, slot]
            live = slot < count_ref[panel, 0]
            which = ident // (nblk * nblk)
            at = pl.ds(pl.multiple_of(slot * TILE, TILE), TILE)
            cols = jnp.concatenate(rows_of(ident % nblk), axis=1)
            half = jnp.dot(blocks_ref[panel, slot], cols, preferred_element_type=jnp.float32)
            half_ref[at, :] = half.astype(jnp.bfloat16)
            rows = rows_of(ident // nblk % nblk)
            keep = [(live & (which == kl)).astype(jnp.float32) for kl in range(KL)]
            for x in range(4):
                turned = rows[x].astype(jnp.float32).T
                for kl in range(KL):
                    left_ref[x, pl.ds(kl * TILE, TILE), at] = (turned * keep[kl]).astype(jnp.bfloat16)
            return carry

        lax.fori_loop(0, slots, one_slot, 0)
        for x in range(4):
            sums = jnp.dot(left_ref[x], half_ref[...], preferred_element_type=jnp.float32)
            groups = sums.reshape(KL, 2, SIDE, 8, sums.shape[1])
            both = jnp.concatenate([groups[0], groups[1]], axis=2).astype(jnp.bfloat16)
            for n in range(2):
                if panel == 0:
                    out_ref[0, 2 * x + n] = both[n]
                else:
                    for zz in range(SIDE):
                        out_ref[1, zz, 2 * x + n] = both[n, zz]


def transform(block_list, block_count, pair_blocks, coef_all):
    panels, slots = pair_blocks.shape[:2]
    nmo = 4 * TILE
    return pl.pallas_call(
        transform_kernel,
        name="transform_blocks",
        out_shape=jax.ShapeDtypeStruct((panels, SIDE, SIDE, KL * 8, nmo), jnp.bfloat16),
        in_specs=[
            pl.BlockSpec(memory_space=pltpu.SMEM),
            pl.BlockSpec(memory_space=pltpu.SMEM),
            pl.BlockSpec(memory_space=pltpu.VMEM),
            pl.BlockSpec(memory_space=pltpu.VMEM),
        ],
        out_specs=pl.BlockSpec(memory_space=pltpu.VMEM),
        scratch_shapes=[
            pltpu.VMEM((slots * TILE, nmo), jnp.bfloat16),
            pltpu.VMEM((4, KL * TILE, slots * TILE), jnp.bfloat16),
        ],
    )(block_list, block_count, pair_blocks, coef_all)


def scatter_kernel(part_ref, out_ref, came, total, final, r_send, r_recv, b_send, b_recv):
    g, p = lax.axis_index("grp"), lax.axis_index("pq")
    y, z = p // SIDE, p % SIDE
    first, second = (y, z), (z, y)
    steps = ((SIDE, 1), (1, SIDE))

    def at(panel, a_to, b_to):
        return (g, a_to * steps[panel][0] + b_to * steps[panel][1])

    barrier = pltpu.get_barrier_semaphore()
    peers = [at(panel, first[panel], (second[panel] + d) % SIDE) for panel in range(2) for d in range(1, 8)]
    for device in peers:
        pl.semaphore_signal(barrier, inc=1, device_id=device, device_id_type=MESH)
    pl.semaphore_wait(barrier, len(peers))

    sent, flights = [], {}

    def hop(panel, way, part, step):
        a = first[panel]
        hops = HALF if way == part else HALF - 1
        away = hops - step
        dest = (a + (away if way == 0 else 8 - away)) % SIDE
        rows = pl.ds(HALF * part, HALF)
        n = ((panel * 2 + way) * 2 + part) * HALF + step
        own = part_ref.at[panel, dest, rows]
        if step > 0:
            held = came.at[n - 1]
            held[...] = (own[...].astype(jnp.float32) + held[...].astype(jnp.float32)).astype(jnp.bfloat16)
        else:
            held = own
        neighbour = at(panel, (a + (1 if way == 0 else 7)) % SIDE, second[panel])
        copy = remote(held, came.at[n], r_send.at[n], r_recv.at[n], neighbour)
        copy.start()
        sent.append(copy)
        flights[panel, way, part, step] = copy

    order = [(panel, way, part) for part in range(2) for panel in range(2) for way in range(2)]
    for panel, way, part in order:
        hop(panel, way, part, 0)
    for step in range(1, HALF + 1):
        for panel, way, part in order:
            hops = HALF if way == part else HALF - 1
            if step <= hops:
                flights[panel, way, part, step - 1].wait_recv()
            if step < hops:
                hop(panel, way, part, step)
    for panel in range(2):
        for part in range(2):
            rows = pl.ds(HALF * part, HALF)
            whole = part_ref[panel, first[panel], rows].astype(jnp.float32)
            for way in range(2):
                hops = HALF if way == part else HALF - 1
                n = ((panel * 2 + way) * 2 + part) * HALF + hops - 1
                whole = whole + came[n].astype(jnp.float32)
            total[panel, rows] = whole.astype(jnp.bfloat16)
    straight = []
    for panel in range(2):
        for d in (4, 3, 5, 2, 6, 1, 7):
            b_to = (second[panel] + d) % SIDE
            n = panel * SIDE + d
            copy = remote(total.at[panel, b_to], final.at[n], b_send.at[n], b_recv.at[n], at(panel, first[panel], b_to))
            copy.start()
            sent.append(copy)
            straight.append(copy)
    for copy in straight:
        copy.wait_recv()
    for panel in range(2):
        rows = total[panel, second[panel]].astype(jnp.float32)
        for d in range(1, 8):
            rows = rows + final[panel * SIDE + d].astype(jnp.float32)
        out_ref[KL * panel] = rows[:8]
        out_ref[KL * panel + 1] = rows[8:]
    for copy in sent:
        copy.wait_send()


def scatter(parts):
    panels, nmo = parts.shape[0], parts.shape[-1]
    return pl.pallas_call(
        scatter_kernel,
        name="reduce_scatter",
        out_shape=jax.ShapeDtypeStruct((panels * KL, 8, nmo), jnp.float32),
        in_specs=[pl.BlockSpec(memory_space=pltpu.VMEM)],
        out_specs=pl.BlockSpec(memory_space=pltpu.VMEM),
        scratch_shapes=[
            pltpu.VMEM((32, HALF, 16, nmo), jnp.bfloat16),
            pltpu.VMEM((2, SIDE, 16, nmo), jnp.bfloat16),
            pltpu.VMEM((2 * SIDE, 16, nmo), jnp.bfloat16),
            pltpu.SemaphoreType.DMA((32,)),
            pltpu.SemaphoreType.DMA((32,)),
            pltpu.SemaphoreType.DMA((16,)),
            pltpu.SemaphoreType.DMA((16,)),
        ],
        compiler_params=pltpu.CompilerParams(collective_id=1, has_side_effects=True),
    )(parts)


def body(pair_blocks, block_list, block_count, coef):
    coef_all = gather(coef)
    parts = transform(block_list, block_count, pair_blocks, coef_all)
    return scatter(parts)


def solution(mesh):
    in_specs = (P("grp", "pq", None, None), P("grp", "pq"), P("grp", "pq"), P("pq", "grp"))
    out_specs = P("grp", "pq", None)
    return jax.shard_map(body, mesh=mesh, in_specs=in_specs, out_specs=out_specs, check_vma=False)
```

```python
import jax
import jax.numpy as jnp
from jax import lax
from jax.experimental import pallas as pl
from jax.experimental.pallas import tpu as pltpu
from jax.sharding import PartitionSpec as P

MESH = pl.DeviceIdType.MESH
SIDE = 8
FAR = SIDE // 2
TILE = 128
KL = 2
BF16 = jnp.bfloat16
NEAR_FIRST = (0, 1, 7, 2, 6, 3, 5, 4)
FAR_FIRST = (4, 3, 5, 2, 6, 1, 7, 0)
PARTS = 4
ROWS = SIDE // PARTS


def near_place(k):
    n = (k + 2 * SIDE - 1) % SIDE
    return 2 * n + 1 + (n // FAR) * (13 - 4 * n)


def far_place(k):
    m = (k + SIDE + FAR) % SIDE
    return 2 * m + (m // FAR) * (15 - 4 * m)


def hops_of(way, part):
    return FAR - (way + part) % 2


def remote(src, dst, send, recv, device):
    return pltpu.make_async_remote_copy(
        src_ref=src, dst_ref=dst, send_sem=send, recv_sem=recv, device_id=device, device_id_type=MESH
    )


def kernel(
    list_ref, count_ref, blocks_hbm, coef_hbm, out_ref,
    own, mine, raw, coef, blocks, half, left, sums, came, total, final,
    in_sem, g_send, g_recv, a_send, a_recv, b_send, b_recv, d_send, d_recv, r_send, r_recv, s_send, s_recv,
):
    g, p = lax.axis_index("grp"), lax.axis_index("pq")
    core = g % 2
    y, z = p // SIDE, p % SIDE
    slots = blocks.shape[1]
    nblk = SIDE * FAR

    barrier = pltpu.get_barrier_semaphore()
    peers = [((g + j) % 8, p) for j in range(1, 8)]
    peers += [(g, (y + d) % SIDE * SIDE + z) for d in range(1, 8)]
    peers += [(g, y * SIDE + (z + d) % SIDE) for d in range(1, 8)]
    for device in peers:
        pl.semaphore_signal(barrier, inc=1, device_id=device, device_id_type=MESH)
    load_coef = pltpu.make_async_copy(coef_hbm, own, in_sem.at[0])
    load_blocks = pltpu.make_async_copy(blocks_hbm, blocks, in_sem.at[1])
    load_coef.start()
    load_blocks.start()
    load_coef.wait()
    mine[...] = jnp.concatenate([own[...], own[...]], axis=1)
    raw[g] = mine[pl.ds(pl.multiple_of(core * 32, 32), 32), :]
    pl.semaphore_wait(barrier, len(peers))

    a = y * (1 - core) + z * core
    b = z * (1 - core) + y * core
    step_a = SIDE * (1 - core) + core
    step_b = (1 - core) + SIDE * core
    partner = (g + 1 - 2 * core, p)
    beside = [(g, a * step_a + (b + 1) % SIDE * step_b), (g, a * step_a + (b + 7) % SIDE * step_b)]

    for j in range(1, 8):
        g_to = (g + j) % 8
        rows = pl.ds(pl.multiple_of((g_to % 2) * 32, 32), 32)
        remote(mine.at[rows, :], raw.at[g], g_send, g_recv, (g_to, p)).start()
    seven = raw.at[pl.ds(0, 7)]
    remote(seven, seven, g_send, g_recv, partner).wait_recv()
    low = lax.broadcasted_iota(jnp.int32, (32, TILE), 1) < TILE // 2
    for x in range(4):
        coef[core, b, 0, x] = jnp.where(low, raw[2 * x], raw[2 * x + 1])

    straight = {}
    for d in NEAR_FIRST[1:]:
        place = NEAR_FIRST.index(SIDE - d)
        to = (g, (a + d) % SIDE * step_a + b * step_b)
        straight[place] = remote(coef.at[core, b, 0], coef.at[core, b, place], a_send, a_recv.at[place], to)
        straight[place].start()

    flights, held = {}, {}

    def send_on(way, place, step):
        away = step if way == 1 else SIDE - step
        b_from = (b + away) % SIDE
        if step < hops_of(way, place):
            piece = coef.at[core, b_from, place]
            copy = remote(piece, piece, b_send, b_recv.at[way, place, step], beside[way])
            copy.start()
            flights[way, place, step + 1] = copy
        if step > 0 or way == 0:
            pair = held.setdefault((away % SIDE, place // 2), set())
            pair.add(place)
            if len(pair) == 2:
                piece = coef.at[core, b_from, pl.ds(place // 2 * 2, 2)]
                remote(piece, piece, d_send, d_recv, partner).start()

    ready = (0.0, 2.2, 2.2, 3.2, 3.2, 4.4, 4.4, 5.6)
    events = sorted(
        (ready[place] + 0.35 * place + 2.6 * step, place, way, step)
        for place in range(SIDE)
        for way in range(2)
        for step in range(hops_of(way, place) + 1)
    )
    for _, place, way, step in events:
        if step > 0:
            flights[way, place, step].wait_recv()
        elif place > 0 and way == 0:
            straight[place].wait_recv()
        send_on(way, place, step)
    remote(coef.at[0], coef.at[0], d_send, d_recv, partner).wait_recv()
    load_blocks.wait()

    def rows_of(tile):
        pieces = []
        for e in range(2):
            y_of, z_of = tile // 4, 2 * (tile % 4) + e
            pieces.append(coef[0, z_of, near_place(y_of - y)])
            pieces.append(coef[1, y_of, near_place(z_of - z)])
        return [jnp.concatenate([piece[x] for piece in pieces], axis=0) for x in range(4)]

    def transform(panel):
        def one_slot(slot, carry):
            ident = list_ref[panel, slot]
            live = slot < count_ref[0, panel]
            which = ident // (nblk * nblk)
            at = pl.ds(pl.multiple_of(slot * TILE, TILE), TILE)
            cols = jnp.concatenate(rows_of(ident % nblk), axis=1)
            half[at, :] = jnp.dot(blocks[panel, slot], cols, preferred_element_type=jnp.float32).astype(BF16)
            rows = rows_of(ident // nblk % nblk)
            keep = [(live & (which == kl)).astype(jnp.float32).astype(BF16) for kl in range(KL)]
            for x in range(4):
                turned = rows[x].T
                for kl in range(KL):
                    left[x, pl.ds(kl * TILE, TILE), at] = turned * keep[kl]
            return carry

        lax.fori_loop(0, slots, one_slot, 0, unroll=3)
        for x in range(4):
            block = jnp.dot(left[x], half[...], preferred_element_type=jnp.float32)
            block = block.reshape(KL, 2, SIDE, 8, block.shape[1])
            block = jnp.concatenate([block[0], block[1]], axis=2).astype(BF16)
            for n in range(2):
                for i in range(SIDE):
                    if panel == 0:
                        sums[0, 2 * x + n, far_place(i - z)] = block[n, i]
                    else:
                        sums[1, i, far_place(2 * x + n - y)] = block[n, i]

    first, second = (y, z), (z, y)
    steps = ((SIDE, 1), (1, SIDE))
    numbers = {}
    for panel in range(2):
        for part in range(PARTS):
            for way in range(2):
                for step in range(hops_of(way, part)):
                    numbers[panel, way, part, step] = len(numbers)
    hopping = {}

    def hop(panel, way, part, step):
        away = hops_of(way, part) - step
        dest = (first[panel] + (away if way == 0 else SIDE - away)) % SIDE
        rows = pl.ds(ROWS * part, ROWS)
        piece = sums.at[panel, dest, rows]
        if step > 0:
            sofar = came.at[numbers[panel, way, part, step - 1]]
            sofar[...] = (piece[...].astype(jnp.float32) + sofar[...].astype(jnp.float32)).astype(BF16)
            piece = sofar
        n = numbers[panel, way, part, step]
        a_to = (first[panel] + (1 if way == 0 else 7)) % SIDE
        to = (g, a_to * steps[panel][0] + second[panel] * steps[panel][1])
        copy = remote(piece, came.at[n], r_send, r_recv.at[n], to)
        copy.start()
        hopping[panel, way, part, step + 1] = copy

    def finish(panel, part):
        rows = pl.ds(ROWS * part, ROWS)
        whole = sums[panel, first[panel], rows].astype(jnp.float32)
        for way in range(2):
            whole = whole + came[numbers[panel, way, part, hops_of(way, part) - 1]].astype(jnp.float32)
        total[panel, rows] = whole.astype(BF16)
        for i in range(ROWS * part, ROWS * part + ROWS):
            d = FAR_FIRST[i]
            if d:
                to = (g, first[panel] * steps[panel][0] + (second[panel] + d) % SIDE * steps[panel][1])
                copy = remote(total.at[panel, i], final.at[panel, i], s_send, s_recv.at[panel], to)
                copy.start()

    for panel in range(2):
        transform(panel)
        for part in range(PARTS):
            for way in range(2):
                hop(panel, way, part, 0)
    for step in range(1, FAR + 1):
        for part in range(PARTS):
            for panel in range(2):
                for way in range(2):
                    if step <= hops_of(way, part):
                        hopping[panel, way, part, step].wait_recv()
                    if step < hops_of(way, part):
                        hop(panel, way, part, step)
                if step == FAR:
                    finish(panel, part)
    for panel in range(2):
        seven = final.at[panel, pl.ds(0, 7)]
        remote(seven, seven, s_send, s_recv.at[panel], partner).wait_recv()
        rows = total[panel, SIDE - 1].astype(jnp.float32)
        for i in range(SIDE - 1):
            rows = rows + final[panel, i].astype(jnp.float32)
        out_ref[KL * panel] = rows[:8]
        out_ref[KL * panel + 1] = rows[8:]

    seven = raw.at[pl.ds(0, 7)]
    remote(seven, seven, g_send, g_recv, partner).wait_send()
    seven = coef.at[0, 0, pl.ds(0, 7)]
    remote(seven, seven, a_send, g_recv, partner).wait_send()
    seven = coef.at[0, pl.ds(0, 7)]
    remote(seven, seven, b_send, g_recv, partner).wait_send()
    remote(coef.at[0], coef.at[0], d_send, d_recv, partner).wait_send()
    remote(came, came, r_send, g_recv, partner).wait_send()
    for panel in range(2):
        seven = final.at[panel, pl.ds(0, 7)]
        remote(seven, seven, s_send, g_recv, partner).wait_send()


def body(pair_blocks, block_list, block_count, coef):
    panels, slots = pair_blocks.shape[:2]
    nmo = 4 * TILE
    dma = pltpu.SemaphoreType.DMA
    return pl.pallas_call(
        kernel,
        name="transform",
        out_shape=jax.ShapeDtypeStruct((panels * KL, 8, nmo), jnp.float32),
        in_specs=[
            pl.BlockSpec(memory_space=pltpu.SMEM),
            pl.BlockSpec(memory_space=pltpu.SMEM),
            pl.BlockSpec(memory_space=pl.ANY),
            pl.BlockSpec(memory_space=pl.ANY),
        ],
        out_specs=pl.BlockSpec(memory_space=pltpu.VMEM),
        scratch_shapes=[
            pltpu.VMEM(coef.shape, BF16),
            pltpu.VMEM((64, TILE), BF16),
            pltpu.VMEM((8, 32, TILE), BF16),
            pltpu.VMEM((2, SIDE, SIDE, 4, 32, TILE), BF16),
            pltpu.VMEM(pair_blocks.shape, BF16),
            pltpu.VMEM((slots * TILE, nmo), BF16),
            pltpu.VMEM((4, KL * TILE, slots * TILE), BF16),
            pltpu.VMEM((panels, SIDE, SIDE, KL * 8, nmo), BF16),
            pltpu.VMEM((2 * PARTS * 7, ROWS, KL * 8, nmo), BF16),
            pltpu.VMEM((panels, SIDE, KL * 8, nmo), BF16),
            pltpu.VMEM((panels, SIDE, KL * 8, nmo), BF16),
            dma((2,)),
            dma,
            dma,
            dma,
            dma((SIDE,)),
            dma,
            dma((2, SIDE, FAR)),
            dma,
            dma,
            dma,
            dma((2 * PARTS * 7,)),
            dma,
            dma((2,)),
        ],
        compiler_params=pltpu.CompilerParams(collective_id=0, has_side_effects=True),
    )(block_list, block_count.reshape(1, panels), pair_blocks, coef)


def solution(mesh):
    in_specs = (P("grp", "pq", None, None), P("grp", "pq"), P("grp", "pq"), P("pq", "grp"))
    out_specs = P("grp", "pq", None)
    return jax.shard_map(body, mesh=mesh, in_specs=in_specs, out_specs=out_specs, check_vma=False)
```

```python
import jax
import jax.numpy as jnp
from jax import lax
from jax.experimental import pallas as pl
from jax.experimental.pallas import tpu as pltpu
from jax.sharding import PartitionSpec as P

MESH = pl.DeviceIdType.MESH
SIDE = 8
FAR = SIDE // 2
TILE = 128
KL = 2
BF16 = jnp.bfloat16
NEAR_FIRST = (0, 1, 7, 2, 6, 3, 5, 4)
FAR_FIRST = (4, 3, 5, 2, 6, 1, 7, 0)
PARTS = 4
ROWS = SIDE // PARTS
UNROLL = 6


def near_place(k):
    n = (k + 2 * SIDE - 1) % SIDE
    return 2 * n + 1 + (n // FAR) * (13 - 4 * n)


def far_place(k):
    m = (k + SIDE + FAR) % SIDE
    return 2 * m + (m // FAR) * (15 - 4 * m)


def hops_of(way, part):
    return FAR - (way + part) % 2


def remote(src, dst, send, recv, device):
    return pltpu.make_async_remote_copy(
        src_ref=src, dst_ref=dst, send_sem=send, recv_sem=recv, device_id=device, device_id_type=MESH
    )


def kernel(
    list_ref, count_ref, blocks_hbm, coef_hbm, out_ref,
    own, mine, theirs, coef, blocks, half, left, sums, came, total, final,
    in_sem, o_send, o_recv, x_send, x_recv, a_send, a_recv, b_send, b_recv, d_send, d_recv, r_send, r_recv, s_send, s_recv,
):
    g, p = lax.axis_index("grp"), lax.axis_index("pq")
    x, core = g // 2, g % 2
    y, z = p // SIDE, p % SIDE
    slots = blocks.shape[1]
    nblk = SIDE * FAR
    first, second = (y, z), (z, y)
    strides = ((SIDE, 1), (1, SIDE))
    partner = (g + 1 - 2 * core, p)

    def at(order, to_first, to_second):
        return (g, to_first % SIDE * strides[order][0] + to_second % SIDE * strides[order][1])

    barrier = pltpu.get_barrier_semaphore()
    peers = [partner] + [((g + 2 * j) % 8, p) for j in range(1, 4)]
    peers += [at(order, first[order] + d, second[order]) for order in range(2) for d in range(1, SIDE)]
    for device in peers:
        pl.semaphore_signal(barrier, inc=1, device_id=device, device_id_type=MESH)
    load_coef = pltpu.make_async_copy(coef_hbm, own, in_sem.at[0])
    load_blocks = pltpu.make_async_copy(blocks_hbm, blocks, in_sem.at[1])
    load_coef.start()
    load_blocks.start()
    load_coef.wait()
    mine[...] = jnp.concatenate([own[...], own[...]], axis=1)
    pl.semaphore_wait(barrier, len(peers))

    @pl.when(core == 0)
    def _():
        hand = remote(mine, theirs, o_send, o_recv, partner)
        hand.start()
        hand.wait_send()
        remote(coef, coef, d_send, d_recv, partner).wait_recv()

    @pl.when(core == 1)
    def _():
        remote(theirs, theirs, o_send, o_recv, partner).wait_recv()
        low = lax.broadcasted_iota(jnp.int32, (64, TILE), 1) < TILE // 2
        both = jnp.where(low, theirs[...], mine[...])
        for order in range(2):
            coef[order, second[order], 0, x] = both[32 * order : 32 * order + 32]
        for j in range(1, 4):
            for order in range(2):
                piece = coef.at[order, second[order], 0, x]
                remote(piece, piece, x_send, x_recv, ((g + 2 * j) % 8, p)).start()
        six = coef.at[0, 0, pl.ds(0, 3), pl.ds(0, 2)]
        remote(six, six, x_send, x_recv, partner).wait_recv()

        straight = {}
        for d in FAR_FIRST[:-1]:
            for order in range(2):
                place = NEAR_FIRST.index(SIDE - d)
                copy = remote(
                    coef.at[order, second[order], 0],
                    coef.at[order, second[order], place],
                    a_send.at[order],
                    a_recv.at[order, place],
                    at(order, first[order] + d, second[order]),
                )
                copy.start()
                straight[order, place] = copy

        flights, held = {}, {}

        def send_on(order, way, place, step):
            away = step if way == 1 else SIDE - step
            row = (second[order] + away) % SIDE
            if step < hops_of(way, place):
                piece = coef.at[order, row, place]
                to = at(order, first[order], second[order] + (1 if way == 0 else 7))
                copy = remote(piece, piece, b_send.at[order], b_recv.at[order, way, place, step], to)
                copy.start()
                flights[order, way, place, step + 1] = copy
            if step > 0 or way == 0:
                pair = held.setdefault((order, away % SIDE, place // 2), set())
                pair.add(place)
                if len(pair) == 2:
                    piece = coef.at[order, row, pl.ds(place // 2 * 2, 2)]
                    remote(piece, piece, d_send, d_recv, partner).start()

        for step in range(FAR + 1):
            for place in range(SIDE):
                for order in range(2):
                    if step == 0 and place > 0:
                        straight[order, place].wait_recv()
                    for way in range(2):
                        if step <= hops_of(way, place):
                            if step > 0:
                                flights[order, way, place, step].wait_recv()
                            send_on(order, way, place, step)
        remote(six, six, x_send, x_recv, partner).wait_send()
        for order in range(2):
            seven = coef.at[0, 0, pl.ds(0, 7)]
            remote(seven, seven, a_send.at[order], d_recv, partner).wait_send()
            seven = coef.at[0, pl.ds(0, 7)]
            remote(seven, seven, b_send.at[order], d_recv, partner).wait_send()
        remote(coef, coef, d_send, d_recv, partner).wait_send()

    load_blocks.wait()

    def rows_of(tile):
        pieces = []
        for e in range(2):
            y_of, z_of = tile // 4, 2 * (tile % 4) + e
            pieces.append(coef[0, z_of, near_place(y_of - y)])
            pieces.append(coef[1, y_of, near_place(z_of - z)])
        return [jnp.concatenate([piece[n] for piece in pieces], axis=0) for n in range(4)]

    def transform(panel):
        def one_slot(slot, carry):
            ident = list_ref[panel, slot]
            live = slot < count_ref[0, panel]
            which = ident // (nblk * nblk)
            here = pl.ds(pl.multiple_of(slot * TILE, TILE), TILE)
            cols = jnp.concatenate(rows_of(ident % nblk), axis=1)
            half[here, :] = jnp.dot(blocks[panel, slot], cols, preferred_element_type=jnp.float32).astype(BF16)
            rows = rows_of(ident // nblk % nblk)
            keep = [(live & (which == kl)).astype(jnp.float32).astype(BF16) for kl in range(KL)]
            for n in range(4):
                turned = rows[n].T
                for kl in range(KL):
                    left[n, pl.ds(kl * TILE, TILE), here] = turned * keep[kl]
            return carry

        lax.fori_loop(0, slots, one_slot, 0, unroll=UNROLL)
        for m in range(4):
            block = jnp.dot(left[m], half[...], preferred_element_type=jnp.float32)
            block = block.reshape(KL, 2, SIDE, 8, block.shape[1])
            block = jnp.concatenate([block[0], block[1]], axis=2).astype(BF16)
            width = block.shape[3] // 2
            for n in range(2):
                for i in range(SIDE):
                    sums[0, 2 * m + n, panel, far_place(i - z)] = block[n, i, :, :width]
                    sums[1, i, panel, far_place(2 * m + n - y)] = block[n, i, :, width:]

    numbers = {}
    for order in range(2):
        for panel in range(2):
            for part in range(PARTS):
                for way in range(2):
                    for step in range(hops_of(way, part)):
                        numbers[order, panel, way, part, step] = len(numbers)
    hopping = {}

    def hop(order, panel, way, part, step):
        away = hops_of(way, part) - step
        dest = (first[order] + (away if way == 0 else SIDE - away)) % SIDE
        piece = sums.at[order, dest, panel, pl.ds(ROWS * part, ROWS)]
        if step > 0:
            sofar = came.at[numbers[order, panel, way, part, step - 1]]
            sofar[...] = (piece[...].astype(jnp.float32) + sofar[...].astype(jnp.float32)).astype(BF16)
            piece = sofar
        n = numbers[order, panel, way, part, step]
        to = at(order, first[order] + (1 if way == 0 else 7), second[order])
        copy = remote(piece, came.at[n], r_send, r_recv.at[n], to)
        copy.start()
        hopping[order, panel, way, part, step + 1] = copy

    def finish(order, panel, part):
        rows = pl.ds(ROWS * part, ROWS)
        whole = sums[order, first[order], panel, rows].astype(jnp.float32)
        for way in range(2):
            whole = whole + came[numbers[order, panel, way, part, hops_of(way, part) - 1]].astype(jnp.float32)
        total[order, panel, rows] = whole.astype(BF16)
        for i in range(ROWS * part, ROWS * part + ROWS):
            if FAR_FIRST[i]:
                to = at(order, first[order], second[order] + FAR_FIRST[i])
                remote(total.at[order, panel, i], final.at[order, panel, i], s_send, s_recv.at[order, panel], to).start()

    for panel in range(2):
        transform(panel)
        for part in range(PARTS):
            for order in range(2):
                for way in range(2):
                    hop(order, panel, way, part, 0)
    for step in range(1, FAR + 1):
        for panel in range(2):
            for part in range(PARTS):
                for order in range(2):
                    for way in range(2):
                        if step <= hops_of(way, part):
                            hopping[order, panel, way, part, step].wait_recv()
                        if step < hops_of(way, part):
                            hop(order, panel, way, part, step)
                    if step == FAR:
                        finish(order, panel, part)
    for panel in range(2):
        for order in range(2):
            seven = final.at[order, panel, pl.ds(0, 7)]
            remote(seven, seven, s_send, s_recv.at[order, panel], partner).wait_recv()
            rows = total[order, panel, SIDE - 1].astype(jnp.float32)
            for i in range(SIDE - 1):
                rows = rows + final[order, panel, i].astype(jnp.float32)
            width = rows.shape[1]
            for kl in range(KL):
                out_ref[KL * panel + kl, :, pl.ds(width * order, width)] = rows[8 * kl : 8 * kl + 8]

    remote(came, came, r_send, d_recv, partner).wait_send()
    seven = final.at[:, :, pl.ds(0, 7)]
    remote(seven, seven, s_send, d_recv, partner).wait_send()


def body(pair_blocks, block_list, block_count, coef):
    panels, slots = pair_blocks.shape[:2]
    nmo = 4 * TILE
    dma = pltpu.SemaphoreType.DMA
    flights = 2 * panels * PARTS * (2 * FAR - 1)
    return pl.pallas_call(
        kernel,
        name="transform",
        out_shape=jax.ShapeDtypeStruct((panels * KL, 8, nmo), jnp.float32),
        in_specs=[
            pl.BlockSpec(memory_space=pltpu.SMEM),
            pl.BlockSpec(memory_space=pltpu.SMEM),
            pl.BlockSpec(memory_space=pl.ANY),
            pl.BlockSpec(memory_space=pl.ANY),
        ],
        out_specs=pl.BlockSpec(memory_space=pltpu.VMEM),
        scratch_shapes=[
            pltpu.VMEM(coef.shape, BF16),
            pltpu.VMEM((64, TILE), BF16),
            pltpu.VMEM((64, TILE), BF16),
            pltpu.VMEM((2, SIDE, SIDE, 4, 32, TILE), BF16),
            pltpu.VMEM(pair_blocks.shape, BF16),
            pltpu.VMEM((slots * TILE, nmo), BF16),
            pltpu.VMEM((4, KL * TILE, slots * TILE), BF16),
            pltpu.VMEM((2, SIDE, panels, SIDE, KL * 8, nmo // 2), BF16),
            pltpu.VMEM((flights, ROWS, KL * 8, nmo // 2), BF16),
            pltpu.VMEM((2, panels, SIDE, KL * 8, nmo // 2), BF16),
            pltpu.VMEM((2, panels, SIDE, KL * 8, nmo // 2), BF16),
            dma((2,)),
            dma,
            dma,
            dma,
            dma,
            dma((2,)),
            dma((2, SIDE)),
            dma((2,)),
            dma((2, 2, SIDE, FAR)),
            dma,
            dma,
            dma,
            dma((flights,)),
            dma,
            dma((2, 2)),
        ],
        compiler_params=pltpu.CompilerParams(collective_id=0, has_side_effects=True),
    )(block_list, block_count.reshape(1, panels), pair_blocks, coef)


def solution(mesh):
    in_specs = (P("grp", "pq", None, None), P("grp", "pq"), P("grp", "pq"), P("pq", "grp"))
    out_specs = P("grp", "pq", None)
    return jax.shard_map(body, mesh=mesh, in_specs=in_specs, out_specs=out_specs, check_vma=False)
```

```python
import jax
import jax.numpy as jnp
from jax import lax
from jax.experimental import pallas as pl
from jax.experimental.pallas import tpu as pltpu
from jax.sharding import PartitionSpec as P

MESH = pl.DeviceIdType.MESH
SIDE = 8
FAR = SIDE // 2
TILE = 128
KL = 2
BF16 = jnp.bfloat16
NEAR_FIRST = (0, 1, 7, 2, 6, 3, 5, 4)
FAR_FIRST = (4, 3, 5, 2, 6, 1, 7, 0)
PARTS = 4
ROWS = SIDE // PARTS
UNROLL = 6
EARLY = ((0,), (1,), (2,), (3,))


def far_place(k):
    m = (k + SIDE + FAR) % SIDE
    return 2 * m + (m // FAR) * (15 - 4 * m)


def hops_of(way, part):
    return FAR - (way + part) % 2


def remote(src, dst, send, recv, device):
    return pltpu.make_async_remote_copy(
        src_ref=src, dst_ref=dst, send_sem=send, recv_sem=recv, device_id=device, device_id_type=MESH
    )


def kernel(
    list_ref, count_ref, blocks_hbm, coef_hbm, out_ref,
    own, mine, theirs, coef, blocks, half, left, sums, came, total, final,
    in_sem, o_send, o_recv, x_send, x_recv, a_send, a_recv, b_send, b_recv, d_send, d_recv, r_send, r_recv, s_send, s_recv,
):
    g, p = lax.axis_index("grp"), lax.axis_index("pq")
    x, core = g // 2, g % 2
    y, z = p // SIDE, p % SIDE
    slots = blocks.shape[1]
    nblk = SIDE * FAR
    first, second = (y, z), (z, y)
    strides = ((SIDE, 1), (1, SIDE))
    partner = (g + 1 - 2 * core, p)

    def at(order, to_first, to_second):
        return (g, to_first % SIDE * strides[order][0] + to_second % SIDE * strides[order][1])

    barrier = pltpu.get_barrier_semaphore()
    peers = [partner] + [((g + 2 * j) % 8, p) for j in range(1, 4)]
    peers += [at(order, first[order] + d, second[order]) for order in range(2) for d in range(1, SIDE)]
    for device in peers:
        pl.semaphore_signal(barrier, inc=1, device_id=device, device_id_type=MESH)
    load_coef = pltpu.make_async_copy(coef_hbm, own, in_sem.at[0])
    load_blocks = pltpu.make_async_copy(blocks_hbm, blocks, in_sem.at[1])
    load_coef.start()
    load_blocks.start()
    load_coef.wait()
    mine[...] = jnp.concatenate([own[...], own[...]], axis=1)
    pl.semaphore_wait(barrier, len(peers))

    @pl.when(core == 0)
    def _():
        hand = remote(mine, theirs, o_send, o_recv, partner)
        hand.start()
        hand.wait_send()
        remote(coef, coef, d_send, d_recv, partner).wait_recv()

    @pl.when(core == 1)
    def _():
        remote(theirs, theirs, o_send, o_recv, partner).wait_recv()
        low = lax.broadcasted_iota(jnp.int32, (64, TILE), 1) < TILE // 2
        both = jnp.where(low, theirs[...], mine[...])
        for order in range(2):
            coef[order, second[order] * SIDE + first[order], x] = both[32 * order : 32 * order + 32]
        for j in range(1, 4):
            for order in range(2):
                piece = coef.at[order, second[order] * SIDE + first[order], x]
                remote(piece, piece, x_send, x_recv, ((g + 2 * j) % 8, p)).start()
        six = coef.at[0, pl.ds(0, 3), pl.ds(0, 2)]
        remote(six, six, x_send, x_recv, partner).wait_recv()

        straight = {}
        for d in FAR_FIRST[:-1]:
            for order in range(2):
                place = NEAR_FIRST.index(SIDE - d)
                piece = coef.at[order, second[order] * SIDE + first[order]]
                to = at(order, first[order] + d, second[order])
                copy = remote(piece, piece, a_send.at[order], a_recv.at[order, place], to)
                copy.start()
                straight[order, place] = copy

        flights = {}

        def send_on(order, way, place, step):
            row = (second[order] + (step if way == 1 else SIDE - step)) % SIDE
            piece = coef.at[order, row * SIDE + (first[order] + NEAR_FIRST[place]) % SIDE]
            if step < hops_of(way, place):
                to = at(order, first[order], second[order] + (1 if way == 0 else 7))
                copy = remote(piece, piece, b_send.at[order], b_recv.at[order, way, place, step], to)
                copy.start()
                flights[order, way, place, step + 1] = copy
            if step > 0 or way == 0:
                remote(piece, piece, d_send, d_recv, partner).start()

        for step in range(FAR + 1):
            for place in range(SIDE):
                for order in range(2):
                    if step == 0 and place > 0:
                        straight[order, place].wait_recv()
                    for way in range(2):
                        if step <= hops_of(way, place):
                            if step > 0:
                                flights[order, way, place, step].wait_recv()
                            send_on(order, way, place, step)
        remote(six, six, x_send, x_recv, partner).wait_send()
        for order in range(2):
            seven = coef.at[0, pl.ds(0, 7)]
            remote(seven, seven, a_send.at[order], d_recv, partner).wait_send()
            seven = coef.at[0, pl.ds(0, 7 * SIDE)]
            remote(seven, seven, b_send.at[order], d_recv, partner).wait_send()
        remote(coef, coef, d_send, d_recv, partner).wait_send()

    load_blocks.wait()

    def rows_of(tile):
        pieces = []
        for e in range(2):
            pieces.append(coef[0, (2 * (tile % 4) + e) * SIDE + tile // 4])
            pieces.append(coef[1, 2 * tile + e])
        return [jnp.concatenate([piece[n] for piece in pieces], axis=0) for n in range(4)]

    def halves(panel):
        def one_slot(slot, carry):
            ident = list_ref[panel, slot]
            live = slot < count_ref[0, panel]
            which = ident // (nblk * nblk)
            here = pl.ds(pl.multiple_of(slot * TILE, TILE), TILE)
            cols = jnp.concatenate(rows_of(ident % nblk), axis=1)
            half[here, :] = jnp.dot(blocks[panel, slot], cols, preferred_element_type=jnp.float32).astype(BF16)
            rows = rows_of(ident // nblk % nblk)
            keep = [(live & (which == kl)).astype(jnp.float32).astype(BF16) for kl in range(KL)]
            for n in range(4):
                turned = rows[n].T
                for kl in range(KL):
                    kept = turned * keep[kl]
                    for i in range(2):
                        left[2 * n + i, pl.ds(kl * 64, 64), here] = kept[64 * i : 64 * i + 64]
            return carry

        lax.fori_loop(0, slots, one_slot, 0, unroll=UNROLL)

    def products(panel, part):
        y_to = [(y + d) % SIDE for d in FAR_FIRST[2 * part : 2 * part + 2]]
        lefts = jnp.concatenate([left[y_to[0]], left[y_to[1]]], axis=0)
        block = jnp.dot(lefts, half[...], preferred_element_type=jnp.float32)
        block = block.reshape(2, KL, SIDE, 8, block.shape[1])
        width = block.shape[4] // 2
        for n in range(2):
            rows = jnp.concatenate([block[n, 0], block[n, 1]], axis=1).astype(BF16)
            for i in range(SIDE):
                sums[0, y_to[n], panel, far_place(i - z)] = rows[i, :, :width]
                sums[1, i, panel, 2 * part + n] = rows[i, :, width:]

    numbers = {}
    for order in range(2):
        for panel in range(2):
            for part in range(PARTS):
                for way in range(2):
                    for step in range(hops_of(way, part)):
                        numbers[order, panel, way, part, step] = len(numbers)
    hopping = {}

    def hop(order, panel, way, part, step):
        away = hops_of(way, part) - step
        dest = (first[order] + (away if way == 0 else SIDE - away)) % SIDE
        piece = sums.at[order, dest, panel, pl.ds(ROWS * part, ROWS)]
        if step > 0:
            sofar = came.at[numbers[order, panel, way, part, step - 1]]
            sofar[...] = (piece[...].astype(jnp.float32) + sofar[...].astype(jnp.float32)).astype(BF16)
            piece = sofar
        n = numbers[order, panel, way, part, step]
        to = at(order, first[order] + (1 if way == 0 else 7), second[order])
        copy = remote(piece, came.at[n], r_send, r_recv.at[n], to)
        copy.start()
        hopping[order, panel, way, part, step + 1] = copy

    def finish(order, panel, part):
        rows = pl.ds(ROWS * part, ROWS)
        whole = sums[order, first[order], panel, rows].astype(jnp.float32)
        for way in range(2):
            whole = whole + came[numbers[order, panel, way, part, hops_of(way, part) - 1]].astype(jnp.float32)
        total[order, panel, rows] = whole.astype(BF16)
        for i in range(ROWS * part, ROWS * part + ROWS):
            if FAR_FIRST[i]:
                to = at(order, first[order], second[order] + FAR_FIRST[i])
                remote(total.at[order, panel, i], final.at[order, panel, i], s_send, s_recv.at[order, panel], to).start()

    def arrive(step, panel, order, parts):
        for part in parts:
            for way in range(2):
                if step <= hops_of(way, part):
                    hopping[order, panel, way, part, step].wait_recv()
                if step < hops_of(way, part):
                    hop(order, panel, way, part, step)
            if step == FAR:
                finish(order, panel, part)

    def leave(panel, part):
        products(panel, part)
        if part < 2:
            for n in range(PARTS):
                for way in range(2):
                    if (way == 1 and hops_of(way, n) < FAR) == (part == 1):
                        hop(0, panel, way, n, 0)
        for way in range(2):
            hop(1, panel, way, part, 0)

    halves(0)
    for part in range(PARTS):
        leave(0, part)
    halves(1)
    arrive(1, 0, 0, range(PARTS))
    for part in range(PARTS):
        arrive(1, 0, 1, EARLY[part])
        leave(1, part)
    for step in range(1, FAR + 1):
        for order in range(2):
            if step < FAR:
                arrive(step + 1, 0, order, range(PARTS))
        for order in range(2):
            arrive(step, 1, order, range(PARTS))
    for panel in range(2):
        for order in range(2):
            seven = final.at[order, panel, pl.ds(0, 7)]
            remote(seven, seven, s_send, s_recv.at[order, panel], partner).wait_recv()
            rows = total[order, panel, SIDE - 1].astype(jnp.float32)
            for i in range(SIDE - 1):
                rows = rows + final[order, panel, i].astype(jnp.float32)
            width = rows.shape[1]
            for kl in range(KL):
                out_ref[KL * panel + kl, :, pl.ds(width * order, width)] = rows[8 * kl : 8 * kl + 8]

    remote(came, came, r_send, d_recv, partner).wait_send()
    seven = final.at[:, :, pl.ds(0, 7)]
    remote(seven, seven, s_send, d_recv, partner).wait_send()


def body(pair_blocks, block_list, block_count, coef):
    panels, slots = pair_blocks.shape[:2]
    nmo = 4 * TILE
    dma = pltpu.SemaphoreType.DMA
    flights = 2 * panels * PARTS * (2 * FAR - 1)
    return pl.pallas_call(
        kernel,
        name="transform",
        out_shape=jax.ShapeDtypeStruct((panels * KL, 8, nmo), jnp.float32),
        in_specs=[
            pl.BlockSpec(memory_space=pltpu.SMEM),
            pl.BlockSpec(memory_space=pltpu.SMEM),
            pl.BlockSpec(memory_space=pl.ANY),
            pl.BlockSpec(memory_space=pl.ANY),
        ],
        out_specs=pl.BlockSpec(memory_space=pltpu.VMEM),
        scratch_shapes=[
            pltpu.VMEM(coef.shape, BF16),
            pltpu.VMEM((64, TILE), BF16),
            pltpu.VMEM((64, TILE), BF16),
            pltpu.VMEM((2, SIDE * SIDE, 4, 32, TILE), BF16),
            pltpu.VMEM(pair_blocks.shape, BF16),
            pltpu.VMEM((slots * TILE, nmo), BF16),
            pltpu.VMEM((SIDE, KL * TILE // 2, slots * TILE), BF16),
            pltpu.VMEM((2, SIDE, panels, SIDE, KL * 8, nmo // 2), BF16),
            pltpu.VMEM((flights, ROWS, KL * 8, nmo // 2), BF16),
            pltpu.VMEM((2, panels, SIDE, KL * 8, nmo // 2), BF16),
            pltpu.VMEM((2, panels, SIDE, KL * 8, nmo // 2), BF16),
            dma((2,)),
            dma,
            dma,
            dma,
            dma,
            dma((2,)),
            dma((2, SIDE)),
            dma((2,)),
            dma((2, 2, SIDE, FAR)),
            dma,
            dma,
            dma,
            dma((flights,)),
            dma,
            dma((2, 2)),
        ],
        compiler_params=pltpu.CompilerParams(collective_id=0, has_side_effects=True),
    )(block_list, block_count.reshape(1, panels), pair_blocks, coef)


def solution(mesh):
    in_specs = (P("grp", "pq", None, None), P("grp", "pq"), P("grp", "pq"), P("pq", "grp"))
    out_specs = P("grp", "pq", None)
    return jax.shard_map(body, mesh=mesh, in_specs=in_specs, out_specs=out_specs, check_vma=False)
```

```python
import jax
import jax.numpy as jnp
from jax import lax
from jax.experimental import pallas as pl
from jax.experimental.pallas import tpu as pltpu
from jax.sharding import PartitionSpec as P

MESH = pl.DeviceIdType.MESH
SIDE = 8
FAR = SIDE // 2
TILE = 128
KL = 2
BF16 = jnp.bfloat16
NEAR_FIRST = (0, 1, 7, 2, 6, 3, 5, 4)
FAR_FIRST = (4, 3, 5, 2, 6, 1, 7, 0)
PARTS = 4
ROWS = SIDE // PARTS
UNROLL = 6
TWO_STAGES = (False, True)
ALL = range(PARTS)
EARLY = ((), ((1, 0, 0, ALL), (1, 0, 1, (0,))), ((1, 0, 1, (1, 2)),), ((1, 0, 1, (3,)),))
LATE = (
    (2, 0, 0), (2, 0, 1), (1, 1, 0), (1, 1, 1), (3, 0, 0), (3, 0, 1),
    (2, 1, 0), (2, 1, 1), (4, 0, 0), (4, 0, 1),
)


def far_place(k):
    m = (k + SIDE + FAR) % SIDE
    return 2 * m + (m // FAR) * (15 - 4 * m)


def hops_of(way, part):
    return FAR - (way + part) % 2


def remote(src, dst, send, recv, device):
    return pltpu.make_async_remote_copy(
        src_ref=src, dst_ref=dst, send_sem=send, recv_sem=recv, device_id=device, device_id_type=MESH
    )


def kernel(
    list_hbm, count_hbm, blocks_hbm, coef_hbm, out_ref,
    list_ref, count_ref, own, mine, theirs, coef, blocks, half, left, sums, came, total, final,
    in_sem, o_send, o_recv, x_send, x_recv, a_send, a_recv, b_send, b_recv, d_send, d_recv, r_send, r_recv, s_send, s_recv,
):
    g, p = lax.axis_index("grp"), lax.axis_index("pq")
    x, core = g // 2, g % 2
    y, z = p // SIDE, p % SIDE
    slots = blocks.shape[1]
    nblk = SIDE * FAR
    first, second = (y, z), (z, y)
    strides = ((SIDE, 1), (1, SIDE))
    partner = (g + 1 - 2 * core, p)

    def at(order, to_first, to_second):
        return (g, to_first % SIDE * strides[order][0] + to_second % SIDE * strides[order][1])

    barrier = pltpu.get_barrier_semaphore()
    peers = [partner] + [((g + 2 * j) % 8, p) for j in range(1, 4)]
    peers += [at(order, first[order] + d, second[order]) for order in range(2) for d in range(1, SIDE)]
    for device in peers:
        pl.semaphore_signal(barrier, inc=1, device_id=device, device_id_type=MESH)
    load_coef = pltpu.make_async_copy(coef_hbm, own, in_sem.at[0])
    load_blocks = pltpu.make_async_copy(blocks_hbm, blocks, in_sem.at[1])
    load_list = pltpu.make_async_copy(list_hbm, list_ref, in_sem.at[2])
    load_count = pltpu.make_async_copy(count_hbm, count_ref, in_sem.at[3])
    load_coef.start()
    load_list.start()
    load_count.start()
    load_blocks.start()
    load_coef.wait()
    mine[...] = jnp.concatenate([own[...], own[...]], axis=1)
    pl.semaphore_wait(barrier, len(peers))

    @pl.when(core == 0)
    def _():
        hand = remote(mine, theirs, o_send, o_recv, partner)
        hand.start()
        hand.wait_send()
        remote(coef, coef, d_send, d_recv, partner).wait_recv()

    @pl.when(core == 1)
    def _():
        remote(theirs, theirs, o_send, o_recv, partner).wait_recv()
        low = lax.broadcasted_iota(jnp.int32, (64, TILE), 1) < TILE // 2
        both = jnp.where(low, theirs[...], mine[...])
        for order in range(2):
            coef[order, second[order] * SIDE + first[order], x] = both[32 * order : 32 * order + 32]
        for j in range(1, 4):
            for order in range(2):
                piece = coef.at[order, second[order] * SIDE + first[order], x]
                remote(piece, piece, x_send, x_recv, ((g + 2 * j) % 8, p)).start()
        six = coef.at[0, pl.ds(0, 3), pl.ds(0, 2)]
        remote(six, six, x_send, x_recv, partner).wait_recv()

        straight = {}
        for d in NEAR_FIRST[1:]:
            for order in range(2):
                place = NEAR_FIRST.index(SIDE - d)
                piece = coef.at[order, second[order] * SIDE + first[order]]
                to = at(order, first[order] + d, second[order])
                copy = remote(piece, piece, a_send.at[order], a_recv.at[order, place], to)
                copy.start()
                straight[order, place] = copy

        flights = {}

        def send_on(order, way, place, step):
            row = (second[order] + (step if way == 1 else SIDE - step)) % SIDE
            piece = coef.at[order, row * SIDE + (first[order] + NEAR_FIRST[place]) % SIDE]
            if step < hops_of(way, place):
                to = at(order, first[order], second[order] + (1 if way == 0 else 7))
                copy = remote(piece, piece, b_send.at[order], b_recv.at[order, way, place, step], to)
                copy.start()
                flights[order, way, place, step + 1] = copy
            if step > 0 or way == 0:
                remote(piece, piece, d_send, d_recv, partner).start()

        for step in range(FAR + 1):
            for place in range(SIDE):
                for order in range(2):
                    if step == 0 and place > 0:
                        straight[order, place].wait_recv()
                    for way in range(2):
                        if step <= hops_of(way, place):
                            if step > 0:
                                flights[order, way, place, step].wait_recv()
                            send_on(order, way, place, step)
        remote(six, six, x_send, x_recv, partner).wait_send()
        for order in range(2):
            seven = coef.at[0, pl.ds(0, 7)]
            remote(seven, seven, a_send.at[order], d_recv, partner).wait_send()
            seven = coef.at[0, pl.ds(0, 7 * SIDE)]
            remote(seven, seven, b_send.at[order], d_recv, partner).wait_send()
        remote(coef, coef, d_send, d_recv, partner).wait_send()

    load_list.wait()
    load_count.wait()
    load_blocks.wait()

    def rows_of(tile):
        pieces = []
        for e in range(2):
            pieces.append(coef[0, (2 * (tile % 4) + e) * SIDE + tile // 4])
            pieces.append(coef[1, 2 * tile + e])
        return [jnp.concatenate([piece[n] for piece in pieces], axis=0) for n in range(4)]

    def halves(panel):
        def one_slot(slot, carry):
            ident = list_ref[panel, slot]
            live = slot < count_ref[0, panel]
            which = ident // (nblk * nblk)
            here = pl.ds(pl.multiple_of(slot * TILE, TILE), TILE)
            cols = jnp.concatenate(rows_of(ident % nblk), axis=1)
            half[here, :] = jnp.dot(blocks[panel, slot], cols, preferred_element_type=jnp.float32).astype(BF16)
            rows = rows_of(ident // nblk % nblk)
            keep = [(live & (which == kl)).astype(jnp.float32).astype(BF16) for kl in range(KL)]
            for n in range(4):
                turned = rows[n].T
                for kl in range(KL):
                    kept = turned * keep[kl]
                    for i in range(2):
                        left[2 * n + i, pl.ds(kl * 64, 64), here] = kept[64 * i : 64 * i + 64]
            return carry

        lax.fori_loop(0, slots, one_slot, 0, unroll=UNROLL)

    def products(panel, part):
        y_to = [(y + d) % SIDE for d in FAR_FIRST[2 * part : 2 * part + 2]]
        lefts = jnp.concatenate([left[y_to[0]], left[y_to[1]]], axis=0)
        block = jnp.dot(lefts, half[...], preferred_element_type=jnp.float32)
        block = block.reshape(2, KL, SIDE, 8, block.shape[1])
        width = block.shape[4] // 2
        for n in range(2):
            rows = jnp.concatenate([block[n, 0], block[n, 1]], axis=1).astype(BF16)
            for i in range(SIDE):
                sums[0, y_to[n], panel, far_place(i - z)] = rows[i, :, :width]
                sums[1, i, panel, 2 * part + n] = rows[i, :, width:]

    numbers, hopping = {}, {}
    for order in range(2):
        for panel in range(2):
            for part in range(PARTS):
                for way in range(2):
                    steps = range(hops_of(way, part))
                    if TWO_STAGES[panel]:
                        steps = ("over", "one", "two") + (("top",) if hops_of(way, part) == FAR else ())
                    for step in steps:
                        numbers[order, panel, way, part, step] = len(numbers)

    def send_sum(key, piece, hops):
        order, _, way, _, _ = key
        to = at(order, first[order] + (hops if way == 0 else SIDE - hops), second[order])
        copy = remote(piece, came.at[numbers[key]], r_send, r_recv.at[numbers[key]], to)
        copy.start()
        hopping[key] = copy

    def sum_for(order, panel, way, part, away):
        dest = (first[order] + (away if way == 0 else SIDE - away)) % SIDE
        return sums.at[order, dest, panel, pl.ds(ROWS * part, ROWS)]

    def added(key, away):
        hopping[key].wait_recv()
        sofar = came.at[numbers[key]]
        piece = sum_for(*key[:4], away)
        sofar[...] = (piece[...].astype(jnp.float32) + sofar[...].astype(jnp.float32)).astype(BF16)
        return sofar

    def finish(order, panel, part):
        rows = pl.ds(ROWS * part, ROWS)
        whole = sums[order, first[order], panel, rows].astype(jnp.float32)
        for way in range(2):
            for step in ("one", "two") if TWO_STAGES[panel] else (hops_of(way, part) - 1,):
                key = (order, panel, way, part, step)
                hopping[key].wait_recv()
                whole = whole + came[numbers[key]].astype(jnp.float32)
        total[order, panel, rows] = whole.astype(BF16)
        for i in range(ROWS * part, ROWS * part + ROWS):
            if FAR_FIRST[i]:
                to = at(order, first[order], second[order] + FAR_FIRST[i])
                remote(total.at[order, panel, i], final.at[order, panel, i], s_send, s_recv.at[order, panel], to).start()

    def arrive(step, panel, order, parts=range(PARTS)):
        last = 2 if TWO_STAGES[panel] else FAR
        for part in parts:
            for way in range(2):
                key = (order, panel, way, part)
                hops = hops_of(way, part)
                if TWO_STAGES[panel]:
                    if step == 1:
                        send_sum((*key, "one"), added((*key, "over"), 1), 1)
                        if hops == FAR:
                            send_sum((*key, "two"), added((*key, "top"), 2), 2)
                elif step < hops:
                    send_sum((*key, step), added((*key, step - 1), hops - step), 1)
            if step == last:
                finish(order, panel, part)

    def begin(order, panel, part, aways):
        for way in range(2):
            key = (order, panel, way, part)
            hops = hops_of(way, part)
            if TWO_STAGES[panel]:
                starts = [("over", 3, 2), ("top", 4, 2) if hops == FAR else ("two", 2, 2)]
            else:
                starts = [(0, hops, 1)]
            for step, away, on in starts:
                if (away if way == 0 else SIDE - away) in aways:
                    send_sum((*key, step), sum_for(*key, away), on)

    def leave(panel, part):
        products(panel, part)
        for n in range(PARTS):
            begin(0, panel, n, FAR_FIRST[2 * part : 2 * part + 2])
        begin(1, panel, part, range(SIDE))

    halves(0)
    for part in range(PARTS):
        leave(0, part)
    halves(1)
    for part in range(PARTS):
        for step, panel, order, parts in EARLY[part]:
            arrive(step, panel, order, parts)
        leave(1, part)
    for step, panel, order in LATE:
        arrive(step, panel, order)
    for panel in range(2):
        for order in range(2):
            seven = final.at[order, panel, pl.ds(0, 7)]
            remote(seven, seven, s_send, s_recv.at[order, panel], partner).wait_recv()
            rows = total[order, panel, SIDE - 1].astype(jnp.float32)
            for i in range(SIDE - 1):
                rows = rows + final[order, panel, i].astype(jnp.float32)
            width = rows.shape[1]
            for kl in range(KL):
                out_ref[KL * panel + kl, :, pl.ds(width * order, width)] = rows[8 * kl : 8 * kl + 8]

    remote(came, came, r_send, d_recv, partner).wait_send()
    seven = final.at[:, :, pl.ds(0, 7)]
    remote(seven, seven, s_send, d_recv, partner).wait_send()


def body(pair_blocks, block_list, block_count, coef):
    panels, slots = pair_blocks.shape[:2]
    nmo = 4 * TILE
    dma = pltpu.SemaphoreType.DMA
    flights = 2 * panels * PARTS * (2 * FAR - 1)
    return pl.pallas_call(
        kernel,
        name="transform",
        out_shape=jax.ShapeDtypeStruct((panels * KL, 8, nmo), jnp.float32),
        in_specs=[
            pl.BlockSpec(memory_space=pl.ANY),
            pl.BlockSpec(memory_space=pl.ANY),
            pl.BlockSpec(memory_space=pl.ANY),
            pl.BlockSpec(memory_space=pl.ANY),
        ],
        out_specs=pl.BlockSpec(memory_space=pltpu.VMEM),
        scratch_shapes=[
            pltpu.SMEM((panels, slots), jnp.int32),
            pltpu.SMEM((1, panels), jnp.int32),
            pltpu.VMEM(coef.shape, BF16),
            pltpu.VMEM((64, TILE), BF16),
            pltpu.VMEM((64, TILE), BF16),
            pltpu.VMEM((2, SIDE * SIDE, 4, 32, TILE), BF16),
            pltpu.VMEM(pair_blocks.shape, BF16),
            pltpu.VMEM((slots * TILE, nmo), BF16),
            pltpu.VMEM((SIDE, KL * TILE // 2, slots * TILE), BF16),
            pltpu.VMEM((2, SIDE, panels, SIDE, KL * 8, nmo // 2), BF16),
            pltpu.VMEM((flights, ROWS, KL * 8, nmo // 2), BF16),
            pltpu.VMEM((2, panels, SIDE, KL * 8, nmo // 2), BF16),
            pltpu.VMEM((2, panels, SIDE, KL * 8, nmo // 2), BF16),
            dma((4,)),
            dma,
            dma,
            dma,
            dma,
            dma((2,)),
            dma((2, SIDE)),
            dma((2,)),
            dma((2, 2, SIDE, FAR)),
            dma,
            dma,
            dma,
            dma((flights,)),
            dma,
            dma((2, 2)),
        ],
        compiler_params=pltpu.CompilerParams(collective_id=0, has_side_effects=True),
    )(block_list, block_count.reshape(1, panels), pair_blocks, coef)


def solution(mesh):
    in_specs = (P("grp", "pq", None, None), P("grp", "pq"), P("grp", "pq"), P("pq", "grp"))
    out_specs = P("grp", "pq", None)
    return jax.shard_map(body, mesh=mesh, in_specs=in_specs, out_specs=out_specs, check_vma=False)
```

```python
import jax
import jax.numpy as jnp
from jax import lax
from jax.experimental import pallas as pl
from jax.experimental.pallas import tpu as pltpu
from jax.sharding import PartitionSpec as P

MESH = pl.DeviceIdType.MESH
SIDE = 8
FAR = SIDE // 2
TILE = 128
KL = 2
BF16 = jnp.bfloat16
NEAR_FIRST = (0, 1, 7, 2, 6, 3, 5, 4)
FAR_FIRST = (4, 3, 5, 2, 6, 1, 7, 0)
PARTS = 4
ROWS = SIDE // PARTS
UNROLL = 9
TWO_STAGES = (False, True)
ALL = range(PARTS)
EARLY = ((), ((1, 0, 0, ALL), (1, 0, 1, (0,))), ((1, 0, 1, (1, 2)),), ((1, 0, 1, (3,)),))
LATE = (
    (2, 0, 0), (2, 0, 1), (1, 1, 0), (1, 1, 1), (3, 0, 0), (3, 0, 1),
    (2, 1, 0), (2, 1, 1), (4, 0, 0), (4, 0, 1),
)


def far_place(k):
    m = (k + SIDE + FAR) % SIDE
    return 2 * m + (m // FAR) * (15 - 4 * m)


def hops_of(way, part):
    return FAR - (way + part) % 2


def remote(src, dst, send, recv, device):
    return pltpu.make_async_remote_copy(
        src_ref=src, dst_ref=dst, send_sem=send, recv_sem=recv, device_id=device, device_id_type=MESH
    )


def kernel(
    list_hbm, count_hbm, blocks_hbm, coef_hbm, out_ref,
    list_ref, count_ref, own, mine, raw, coef, blocks, half, left, sums, came, total, final,
    in_sem, o_send, o_recv, a_send, a_recv, b_send, b_recv, d_send, d_recv, r_send, r_recv, s_send, s_recv,
):
    g, p = lax.axis_index("grp"), lax.axis_index("pq")
    x, core = g // 2, g % 2
    y, z = p // SIDE, p % SIDE
    slots = blocks.shape[1]
    nblk = SIDE * FAR
    first, second = (y, z), (z, y)
    strides = ((SIDE, 1), (1, SIDE))
    partner = (g + 1 - 2 * core, p)

    def at(order, to_first, to_second):
        return (g, to_first % SIDE * strides[order][0] + to_second % SIDE * strides[order][1])

    barrier = pltpu.get_barrier_semaphore()
    peers = [((g + j) % 8, p) for j in range(1, 8)]
    peers += [at(order, first[order] + d, second[order]) for order in range(2) for d in range(1, SIDE)]
    for device in peers:
        pl.semaphore_signal(barrier, inc=1, device_id=device, device_id_type=MESH)
    load_coef = pltpu.make_async_copy(coef_hbm, own, in_sem.at[0])
    load_blocks = pltpu.make_async_copy(blocks_hbm, blocks, in_sem.at[1])
    load_list = pltpu.make_async_copy(list_hbm, list_ref, in_sem.at[2])
    load_count = pltpu.make_async_copy(count_hbm, count_ref, in_sem.at[3])
    load_coef.start()
    load_list.start()
    load_count.start()
    load_blocks.start()
    load_coef.wait()
    mine[...] = jnp.concatenate([own[...], own[...]], axis=1)
    pl.semaphore_wait(barrier, len(peers))

    @pl.when(core == 0)
    def _():
        for j in (1, 3, 5, 7):
            remote(mine, raw.at[g], o_send, o_recv, ((g + j) % 8, p)).start()
        remote(coef, coef, d_send, d_recv, partner).wait_recv()

    @pl.when(core == 1)
    def _():
        for j in (2, 4, 6):
            remote(mine, raw.at[g], o_send, o_recv, ((g + j) % 8, p)).start()
        raw[g] = mine[...]
        seven = raw.at[pl.ds(0, 7)]
        remote(seven, seven, o_send, o_recv, partner).wait_recv()
        low = lax.broadcasted_iota(jnp.int32, (64, TILE), 1) < TILE // 2
        for n in range(4):
            both = jnp.where(low, raw[2 * n], raw[2 * n + 1])
            for order in range(2):
                coef[order, second[order] * SIDE + first[order], n] = both[32 * order : 32 * order + 32]

        straight = {}
        for d in NEAR_FIRST[1:]:
            for order in range(2):
                place = NEAR_FIRST.index(SIDE - d)
                piece = coef.at[order, second[order] * SIDE + first[order]]
                to = at(order, first[order] + d, second[order])
                copy = remote(piece, piece, a_send.at[order], a_recv.at[order, place], to)
                copy.start()
                straight[order, place] = copy

        flights = {}

        def send_on(order, way, place, step):
            row = (second[order] + (step if way == 1 else SIDE - step)) % SIDE
            piece = coef.at[order, row * SIDE + (first[order] + NEAR_FIRST[place]) % SIDE]
            if step < hops_of(way, place):
                to = at(order, first[order], second[order] + (1 if way == 0 else 7))
                copy = remote(piece, piece, b_send.at[order], b_recv.at[order, way, place, step], to)
                copy.start()
                flights[order, way, place, step + 1] = copy
            if step > 0 or way == 0:
                remote(piece, piece, d_send, d_recv, partner).start()

        for step in range(FAR + 1):
            for place in range(SIDE):
                for order in range(2):
                    if step == 0 and place > 0:
                        straight[order, place].wait_recv()
                    for way in range(2):
                        if step <= hops_of(way, place):
                            if step > 0:
                                flights[order, way, place, step].wait_recv()
                            send_on(order, way, place, step)

    load_list.wait()
    load_count.wait()
    load_blocks.wait()

    def rows_of(tile):
        pieces = []
        for e in range(2):
            pieces.append(coef[0, (2 * (tile % 4) + e) * SIDE + tile // 4])
            pieces.append(coef[1, 2 * tile + e])
        return [jnp.concatenate([piece[n] for piece in pieces], axis=0) for n in range(4)]

    def halves(panel):
        def one_slot(slot, carry):
            ident = list_ref[panel, slot]
            live = slot < count_ref[0, panel]
            which = ident // (nblk * nblk)
            here = pl.ds(pl.multiple_of(slot * TILE, TILE), TILE)
            cols = jnp.concatenate(rows_of(ident % nblk), axis=1)
            half[here, :] = jnp.dot(blocks[panel, slot], cols, preferred_element_type=jnp.float32).astype(BF16)
            rows = rows_of(ident // nblk % nblk)
            keep = [(live & (which == kl)).astype(jnp.float32).astype(BF16) for kl in range(KL)]
            for n in range(4):
                turned = rows[n].T
                for kl in range(KL):
                    kept = turned * keep[kl]
                    for i in range(2):
                        left[2 * n + i, pl.ds(kl * 64, 64), here] = kept[64 * i : 64 * i + 64]
            return carry

        lax.fori_loop(0, slots, one_slot, 0, unroll=UNROLL)

    def products(panel, part):
        y_to = [(y + d) % SIDE for d in FAR_FIRST[2 * part : 2 * part + 2]]
        lefts = jnp.concatenate([left[y_to[0]], left[y_to[1]]], axis=0)
        block = jnp.dot(lefts, half[...], preferred_element_type=jnp.float32)
        block = block.reshape(2, KL, SIDE, 8, block.shape[1])
        width = block.shape[4] // 2
        for n in range(2):
            rows = jnp.concatenate([block[n, 0], block[n, 1]], axis=1).astype(BF16)
            for i in range(SIDE):
                sums[0, y_to[n], panel, far_place(i - z)] = rows[i, :, :width]
                sums[1, i, panel, 2 * part + n] = rows[i, :, width:]

    numbers, hopping = {}, {}
    for order in range(2):
        for panel in range(2):
            for part in range(PARTS):
                for way in range(2):
                    steps = range(hops_of(way, part))
                    if TWO_STAGES[panel]:
                        steps = ("over", "one", "two") + (("top",) if hops_of(way, part) == FAR else ())
                    for step in steps:
                        numbers[order, panel, way, part, step] = len(numbers)

    def send_sum(key, piece, hops):
        order, _, way, _, _ = key
        to = at(order, first[order] + (hops if way == 0 else SIDE - hops), second[order])
        copy = remote(piece, came.at[numbers[key]], r_send, r_recv.at[numbers[key]], to)
        copy.start()
        hopping[key] = copy

    def sum_for(order, panel, way, part, away):
        dest = (first[order] + (away if way == 0 else SIDE - away)) % SIDE
        return sums.at[order, dest, panel, pl.ds(ROWS * part, ROWS)]

    def added(key, away):
        hopping[key].wait_recv()
        sofar = came.at[numbers[key]]
        piece = sum_for(*key[:4], away)
        sofar[...] = (piece[...].astype(jnp.float32) + sofar[...].astype(jnp.float32)).astype(BF16)
        return sofar

    def finish(order, panel, part):
        rows = pl.ds(ROWS * part, ROWS)
        whole = sums[order, first[order], panel, rows].astype(jnp.float32)
        for way in range(2):
            for step in ("one", "two") if TWO_STAGES[panel] else (hops_of(way, part) - 1,):
                key = (order, panel, way, part, step)
                hopping[key].wait_recv()
                whole = whole + came[numbers[key]].astype(jnp.float32)
        total[order, panel, rows] = whole.astype(BF16)
        for i in range(ROWS * part, ROWS * part + ROWS):
            if FAR_FIRST[i]:
                to = at(order, first[order], second[order] + FAR_FIRST[i])
                remote(total.at[order, panel, i], final.at[order, panel, i], s_send, s_recv.at[order, panel], to).start()

    def arrive(step, panel, order, parts=range(PARTS)):
        last = 2 if TWO_STAGES[panel] else FAR
        for part in parts:
            for way in range(2):
                key = (order, panel, way, part)
                hops = hops_of(way, part)
                if TWO_STAGES[panel]:
                    if step == 1:
                        send_sum((*key, "one"), added((*key, "over"), 1), 1)
                        if hops == FAR:
                            send_sum((*key, "two"), added((*key, "top"), 2), 2)
                elif step < hops:
                    send_sum((*key, step), added((*key, step - 1), hops - step), 1)
            if step == last:
                finish(order, panel, part)

    def begin(order, panel, part, aways):
        for way in range(2):
            key = (order, panel, way, part)
            hops = hops_of(way, part)
            if TWO_STAGES[panel]:
                starts = [("over", 3, 2), ("top", 4, 2) if hops == FAR else ("two", 2, 2)]
            else:
                starts = [(0, hops, 1)]
            for step, away, on in starts:
                if (away if way == 0 else SIDE - away) in aways:
                    send_sum((*key, step), sum_for(*key, away), on)

    def leave(panel, part):
        products(panel, part)
        for n in range(PARTS):
            begin(0, panel, n, FAR_FIRST[2 * part : 2 * part + 2])
        begin(1, panel, part, range(SIDE))

    halves(0)
    for part in range(PARTS):
        leave(0, part)
    halves(1)
    for part in range(PARTS):
        for step, panel, order, parts in EARLY[part]:
            arrive(step, panel, order, parts)
        leave(1, part)
    for step, panel, order in LATE:
        arrive(step, panel, order)
    for panel in range(2):
        for order in range(2):
            seven = final.at[order, panel, pl.ds(0, 7)]
            remote(seven, seven, s_send, s_recv.at[order, panel], partner).wait_recv()
            rows = total[order, panel, SIDE - 1].astype(jnp.float32)
            for i in range(SIDE - 1):
                rows = rows + final[order, panel, i].astype(jnp.float32)
            width = rows.shape[1]
            for kl in range(KL):
                out_ref[KL * panel + kl, :, pl.ds(width * order, width)] = rows[8 * kl : 8 * kl + 8]

    @pl.when(core == 0)
    def _():
        four = raw.at[pl.ds(0, 4)]
        remote(four, four, o_send, d_recv, partner).wait_send()

    @pl.when(core == 1)
    def _():
        three = raw.at[pl.ds(0, 3)]
        remote(three, three, o_send, d_recv, partner).wait_send()
        for order in range(2):
            seven = coef.at[0, pl.ds(0, 7)]
            remote(seven, seven, a_send.at[order], d_recv, partner).wait_send()
            seven = coef.at[0, pl.ds(0, 7 * SIDE)]
            remote(seven, seven, b_send.at[order], d_recv, partner).wait_send()
        remote(coef, coef, d_send, d_recv, partner).wait_send()

    remote(came, came, r_send, d_recv, partner).wait_send()
    seven = final.at[:, :, pl.ds(0, 7)]
    remote(seven, seven, s_send, d_recv, partner).wait_send()


def body(pair_blocks, block_list, block_count, coef):
    panels, slots = pair_blocks.shape[:2]
    nmo = 4 * TILE
    dma = pltpu.SemaphoreType.DMA
    flights = 2 * panels * PARTS * (2 * FAR - 1)
    return pl.pallas_call(
        kernel,
        name="transform",
        out_shape=jax.ShapeDtypeStruct((panels * KL, 8, nmo), jnp.float32),
        in_specs=[
            pl.BlockSpec(memory_space=pl.ANY),
            pl.BlockSpec(memory_space=pl.ANY),
            pl.BlockSpec(memory_space=pl.ANY),
            pl.BlockSpec(memory_space=pl.ANY),
        ],
        out_specs=pl.BlockSpec(memory_space=pltpu.VMEM),
        scratch_shapes=[
            pltpu.SMEM((panels, slots), jnp.int32),
            pltpu.SMEM((1, panels), jnp.int32),
            pltpu.VMEM(coef.shape, BF16),
            pltpu.VMEM((64, TILE), BF16),
            pltpu.VMEM((8, 64, TILE), BF16),
            pltpu.VMEM((2, SIDE * SIDE, 4, 32, TILE), BF16),
            pltpu.VMEM(pair_blocks.shape, BF16),
            pltpu.VMEM((slots * TILE, nmo), BF16),
            pltpu.VMEM((SIDE, KL * TILE // 2, slots * TILE), BF16),
            pltpu.VMEM((2, SIDE, panels, SIDE, KL * 8, nmo // 2), BF16),
            pltpu.VMEM((flights, ROWS, KL * 8, nmo // 2), BF16),
            pltpu.VMEM((2, panels, SIDE, KL * 8, nmo // 2), BF16),
            pltpu.VMEM((2, panels, SIDE, KL * 8, nmo // 2), BF16),
            dma((4,)),
            dma,
            dma,
            dma((2,)),
            dma((2, SIDE)),
            dma((2,)),
            dma((2, 2, SIDE, FAR)),
            dma,
            dma,
            dma,
            dma((flights,)),
            dma,
            dma((2, 2)),
        ],
        compiler_params=pltpu.CompilerParams(collective_id=0, has_side_effects=True),
    )(block_list, block_count.reshape(1, panels), pair_blocks, coef)


def solution(mesh):
    in_specs = (P("grp", "pq", None, None), P("grp", "pq"), P("grp", "pq"), P("pq", "grp"))
    out_specs = P("grp", "pq", None)
    return jax.shard_map(body, mesh=mesh, in_specs=in_specs, out_specs=out_specs, check_vma=False)
```

```python
import jax
import jax.numpy as jnp
from jax import lax
from jax.experimental import pallas as pl
from jax.experimental.pallas import tpu as pltpu
from jax.sharding import PartitionSpec as P

MESH = pl.DeviceIdType.MESH
SIDE = 8
FAR = SIDE // 2
TILE = 128
KL = 2
BF16 = jnp.bfloat16
NEAR_FIRST = (0, 1, 7, 2, 6, 3, 5, 4)
FAR_FIRST = (4, 3, 5, 2, 6, 1, 7, 0)
PARTS = 4
ROWS = SIDE // PARTS
UNROLL = 9
TWO_STAGES = (False, True)
ALL = range(PARTS)
EARLY = (((1, 0, 0, ALL),), ((1, 0, 1, (0, 1)),), ((1, 0, 1, (2,)),), ((1, 0, 1, (3,)),))
LATE = (
    (2, 0, 0), (2, 0, 1), (1, 1, 0), (1, 1, 1), (3, 0, 0), (3, 0, 1),
    (2, 1, 0), (2, 1, 1), (4, 0, 0), (4, 0, 1),
)


def far_place(k):
    m = (k + SIDE + FAR) % SIDE
    return 2 * m + (m // FAR) * (15 - 4 * m)


def hops_of(way, part):
    return FAR - (way + part) % 2


def remote(src, dst, send, recv, device):
    return pltpu.make_async_remote_copy(
        src_ref=src, dst_ref=dst, send_sem=send, recv_sem=recv, device_id=device, device_id_type=MESH
    )


def kernel(
    list_hbm, count_hbm, blocks_hbm, coef_hbm, out_ref,
    list_ref, count_ref, own, mine, raw, coef, blocks, half, left, sums, came, total, final,
    in_sem, o_send, o_recv, a_send, a_recv, b_send, b_recv, d_send, d_recv, r_send, r_recv, s_send, s_recv,
):
    g, p = lax.axis_index("grp"), lax.axis_index("pq")
    x, core = g // 2, g % 2
    y, z = p // SIDE, p % SIDE
    slots = blocks.shape[1]
    nblk = SIDE * FAR
    first, second = (y, z), (z, y)
    strides = ((SIDE, 1), (1, SIDE))
    partner = (g + 1 - 2 * core, p)

    def at(order, to_first, to_second):
        return (g, to_first % SIDE * strides[order][0] + to_second % SIDE * strides[order][1])

    barrier = pltpu.get_barrier_semaphore()
    peers = [((g + j) % 8, p) for j in range(1, 8)]
    peers += [at(order, first[order] + d, second[order]) for order in range(2) for d in range(1, SIDE)]
    for device in peers:
        pl.semaphore_signal(barrier, inc=1, device_id=device, device_id_type=MESH)
    load_coef = pltpu.make_async_copy(coef_hbm, own, in_sem.at[0])
    load_blocks = pltpu.make_async_copy(blocks_hbm, blocks, in_sem.at[1])
    load_list = pltpu.make_async_copy(list_hbm, list_ref, in_sem.at[2])
    load_count = pltpu.make_async_copy(count_hbm, count_ref, in_sem.at[3])
    load_coef.start()
    load_list.start()
    load_count.start()
    load_blocks.start()
    load_coef.wait()
    mine[...] = jnp.concatenate([own[...], own[...]], axis=1)
    pl.semaphore_wait(barrier, len(peers))

    @pl.when(core == 0)
    def _():
        for j in (1, 3, 5, 7):
            remote(mine, raw.at[g], o_send, o_recv, ((g + j) % 8, p)).start()
        remote(coef, coef, d_send, d_recv, partner).wait_recv()

    @pl.when(core == 1)
    def _():
        for j in (2, 4, 6):
            remote(mine, raw.at[g], o_send, o_recv, ((g + j) % 8, p)).start()
        raw[g] = mine[...]
        seven = raw.at[pl.ds(0, 7)]
        remote(seven, seven, o_send, o_recv, partner).wait_recv()
        low = lax.broadcasted_iota(jnp.int32, (64, TILE), 1) < TILE // 2
        for n in range(4):
            both = jnp.where(low, raw[2 * n], raw[2 * n + 1])
            for order in range(2):
                coef[order, second[order] * SIDE + first[order], n] = both[32 * order : 32 * order + 32]

        straight = {}
        for d in NEAR_FIRST[1:]:
            for order in range(2):
                place = NEAR_FIRST.index(SIDE - d)
                piece = coef.at[order, second[order] * SIDE + first[order]]
                to = at(order, first[order] + d, second[order])
                copy = remote(piece, piece, a_send.at[order], a_recv.at[order, place], to)
                copy.start()
                straight[order, place] = copy

        flights = {}

        def send_on(order, way, place, step):
            row = (second[order] + (step if way == 1 else SIDE - step)) % SIDE
            piece = coef.at[order, row * SIDE + (first[order] + NEAR_FIRST[place]) % SIDE]
            if step < hops_of(way, place):
                to = at(order, first[order], second[order] + (1 if way == 0 else 7))
                copy = remote(piece, piece, b_send.at[order], b_recv.at[order, way, place, step], to)
                copy.start()
                flights[order, way, place, step + 1] = copy
            if step > 0 or way == 0:
                remote(piece, piece, d_send, d_recv, partner).start()

        for step in range(FAR + 1):
            for place in range(SIDE):
                for order in range(2):
                    if step == 0 and place > 0:
                        straight[order, place].wait_recv()
                    for way in range(2):
                        if step <= hops_of(way, place):
                            if step > 0:
                                flights[order, way, place, step].wait_recv()
                            send_on(order, way, place, step)

    load_list.wait()
    load_count.wait()
    load_blocks.wait()

    def rows_of(tile):
        pieces = []
        for e in range(2):
            pieces.append(coef[0, (2 * (tile % 4) + e) * SIDE + tile // 4])
            pieces.append(coef[1, 2 * tile + e])
        return [jnp.concatenate([piece[n] for piece in pieces], axis=0) for n in range(4)]

    def halves(panel):
        def one_slot(slot, carry):
            ident = list_ref[panel, slot]
            live = slot < count_ref[0, panel]
            which = ident // (nblk * nblk)
            here = pl.ds(pl.multiple_of(slot * TILE, TILE), TILE)
            cols = jnp.concatenate(rows_of(ident % nblk), axis=1)
            half[here, :] = jnp.dot(blocks[panel, slot], cols, preferred_element_type=jnp.float32).astype(BF16)
            rows = rows_of(ident // nblk % nblk)
            keep = [(live & (which == kl)).astype(jnp.float32).astype(BF16) for kl in range(KL)]
            for n in range(4):
                turned = rows[n].T
                for kl in range(KL):
                    kept = turned * keep[kl]
                    for i in range(2):
                        left[2 * n + i, pl.ds(kl * 64, 64), here] = kept[64 * i : 64 * i + 64]
            return carry

        lax.fori_loop(0, slots, one_slot, 0, unroll=UNROLL)

    def products(panel, part):
        y_to = [(y + d) % SIDE for d in FAR_FIRST[2 * part : 2 * part + 2]]
        lefts = jnp.concatenate([left[y_to[0]], left[y_to[1]]], axis=0)
        block = jnp.dot(lefts, half[...], preferred_element_type=jnp.float32)
        block = block.reshape(2, KL, SIDE, 8, block.shape[1])
        width = block.shape[4] // 2
        for n in range(2):
            rows = jnp.concatenate([block[n, 0], block[n, 1]], axis=1).astype(BF16)
            for i in range(SIDE):
                sums[0, y_to[n], panel, far_place(i - z)] = rows[i, :, :width]
                sums[1, i, panel, 2 * part + n] = rows[i, :, width:]

    numbers, hopping = {}, {}
    for order in range(2):
        for panel in range(2):
            for part in range(PARTS):
                for way in range(2):
                    steps = range(hops_of(way, part))
                    if TWO_STAGES[panel]:
                        steps = ("over", "one", "two") + (("top",) if hops_of(way, part) == FAR else ())
                    for step in steps:
                        numbers[order, panel, way, part, step] = len(numbers)

    def send_sum(key, piece, hops):
        order, _, way, _, _ = key
        to = at(order, first[order] + (hops if way == 0 else SIDE - hops), second[order])
        copy = remote(piece, came.at[numbers[key]], r_send, r_recv.at[numbers[key]], to)
        copy.start()
        hopping[key] = copy

    def sum_for(order, panel, way, part, away):
        dest = (first[order] + (away if way == 0 else SIDE - away)) % SIDE
        return sums.at[order, dest, panel, pl.ds(ROWS * part, ROWS)]

    def added(key, away):
        hopping[key].wait_recv()
        sofar = came.at[numbers[key]]
        piece = sum_for(*key[:4], away)
        sofar[...] = (piece[...].astype(jnp.float32) + sofar[...].astype(jnp.float32)).astype(BF16)
        return sofar

    def finish(order, panel, part):
        rows = pl.ds(ROWS * part, ROWS)
        whole = sums[order, first[order], panel, rows].astype(jnp.float32)
        for way in range(2):
            for step in ("one", "two") if TWO_STAGES[panel] else (hops_of(way, part) - 1,):
                key = (order, panel, way, part, step)
                hopping[key].wait_recv()
                whole = whole + came[numbers[key]].astype(jnp.float32)
        total[order, panel, rows] = whole.astype(BF16)
        for i in range(ROWS * part, ROWS * part + ROWS):
            if FAR_FIRST[i]:
                to = at(order, first[order], second[order] + FAR_FIRST[i])
                remote(total.at[order, panel, i], final.at[order, panel, i], s_send, s_recv.at[order, panel], to).start()

    def arrive(step, panel, order, parts=range(PARTS)):
        last = 2 if TWO_STAGES[panel] else FAR
        for part in parts:
            for way in range(2):
                key = (order, panel, way, part)
                hops = hops_of(way, part)
                if TWO_STAGES[panel]:
                    if step == 1:
                        send_sum((*key, "one"), added((*key, "over"), 1), 1)
                        if hops == FAR:
                            send_sum((*key, "two"), added((*key, "top"), 2), 2)
                elif step < hops:
                    send_sum((*key, step), added((*key, step - 1), hops - step), 1)
            if step == last:
                finish(order, panel, part)

    def begin(order, panel, part, aways):
        for way in range(2):
            key = (order, panel, way, part)
            hops = hops_of(way, part)
            if TWO_STAGES[panel]:
                starts = [("over", 3, 2), ("top", 4, 2) if hops == FAR else ("two", 2, 2)]
            else:
                starts = [(0, hops, 1)]
            for step, away, on in starts:
                if (away if way == 0 else SIDE - away) in aways:
                    send_sum((*key, step), sum_for(*key, away), on)

    def leave(panel, part):
        products(panel, part)
        for n in range(PARTS):
            begin(0, panel, n, FAR_FIRST[2 * part : 2 * part + 2])
        begin(1, panel, part, range(SIDE))

    halves(0)
    for part in range(PARTS):
        leave(0, part)
    halves(1)
    for part in range(PARTS):
        for step, panel, order, parts in EARLY[part]:
            arrive(step, panel, order, parts)
        leave(1, part)
    for step, panel, order in LATE:
        arrive(step, panel, order)
    for panel in range(2):
        for order in range(2):
            seven = final.at[order, panel, pl.ds(0, 7)]
            remote(seven, seven, s_send, s_recv.at[order, panel], partner).wait_recv()
            rows = total[order, panel, SIDE - 1].astype(jnp.float32)
            for i in range(SIDE - 1):
                rows = rows + final[order, panel, i].astype(jnp.float32)
            width = rows.shape[1]
            for kl in range(KL):
                out_ref[KL * panel + kl, :, pl.ds(width * order, width)] = rows[8 * kl : 8 * kl + 8]

    @pl.when(core == 0)
    def _():
        four = raw.at[pl.ds(0, 4)]
        remote(four, four, o_send, d_recv, partner).wait_send()

    @pl.when(core == 1)
    def _():
        three = raw.at[pl.ds(0, 3)]
        remote(three, three, o_send, d_recv, partner).wait_send()
        for order in range(2):
            seven = coef.at[0, pl.ds(0, 7)]
            remote(seven, seven, a_send.at[order], d_recv, partner).wait_send()
            seven = coef.at[0, pl.ds(0, 7 * SIDE)]
            remote(seven, seven, b_send.at[order], d_recv, partner).wait_send()
        remote(coef, coef, d_send, d_recv, partner).wait_send()

    remote(came, came, r_send, d_recv, partner).wait_send()
    seven = final.at[:, :, pl.ds(0, 7)]
    remote(seven, seven, s_send, d_recv, partner).wait_send()


def body(pair_blocks, block_list, block_count, coef):
    panels, slots = pair_blocks.shape[:2]
    nmo = 4 * TILE
    dma = pltpu.SemaphoreType.DMA
    flights = 2 * panels * PARTS * (2 * FAR - 1)
    return pl.pallas_call(
        kernel,
        name="transform",
        out_shape=jax.ShapeDtypeStruct((panels * KL, 8, nmo), jnp.float32),
        in_specs=[
            pl.BlockSpec(memory_space=pl.ANY),
            pl.BlockSpec(memory_space=pl.ANY),
            pl.BlockSpec(memory_space=pl.ANY),
            pl.BlockSpec(memory_space=pl.ANY),
        ],
        out_specs=pl.BlockSpec(memory_space=pltpu.VMEM),
        scratch_shapes=[
            pltpu.SMEM((panels, slots), jnp.int32),
            pltpu.SMEM((1, panels), jnp.int32),
            pltpu.VMEM(coef.shape, BF16),
            pltpu.VMEM((64, TILE), BF16),
            pltpu.VMEM((8, 64, TILE), BF16),
            pltpu.VMEM((2, SIDE * SIDE, 4, 32, TILE), BF16),
            pltpu.VMEM(pair_blocks.shape, BF16),
            pltpu.VMEM((slots * TILE, nmo), BF16),
            pltpu.VMEM((SIDE, KL * TILE // 2, slots * TILE), BF16),
            pltpu.VMEM((2, SIDE, panels, SIDE, KL * 8, nmo // 2), BF16),
            pltpu.VMEM((flights, ROWS, KL * 8, nmo // 2), BF16),
            pltpu.VMEM((2, panels, SIDE, KL * 8, nmo // 2), BF16),
            pltpu.VMEM((2, panels, SIDE, KL * 8, nmo // 2), BF16),
            dma((4,)),
            dma,
            dma,
            dma((2,)),
            dma((2, SIDE)),
            dma((2,)),
            dma((2, 2, SIDE, FAR)),
            dma,
            dma,
            dma,
            dma((flights,)),
            dma,
            dma((2, 2)),
        ],
        compiler_params=pltpu.CompilerParams(collective_id=0, has_side_effects=True),
    )(block_list, block_count.reshape(1, panels), pair_blocks, coef)


def solution(mesh):
    in_specs = (P("grp", "pq", None, None), P("grp", "pq"), P("grp", "pq"), P("pq", "grp"))
    out_specs = P("grp", "pq", None)
    return jax.shard_map(body, mesh=mesh, in_specs=in_specs, out_specs=out_specs, check_vma=False)
```
